16 devices in a mesh: dp: 1, ep: 16 (over x, y, z, core).
Axes of the slice: x: 2, y: 2, z: 2, core: 2. Of those that a mesh axis runs over, the one named last changes fastest.
Arguments:
- x: bfloat16 [1, 16, 256, 3584], P('dp', 'ep')
- expert: int32 [1, 16, 256, 8], P('dp', 'ep')
- slot: int32 [1, 16, 256, 8], P('dp', 'ep')
- gate: float32 [1, 16, 256, 8], P('dp', 'ep')
- w_gate: bfloat16 [48, 3584, 2048], P('ep')
- w_up: bfloat16 [48, 3584, 2048], P('ep')
- w_down: bfloat16 [48, 2048, 3584], P('ep')
- s_gate: bfloat16 [3584, 2048], replicated
- s_up: bfloat16 [3584, 2048], replicated
- s_down: bfloat16 [2048, 3584], replicated
Outputs:
- y: bfloat16 [1, 16, 256, 3584], P('dp', 'ep')
All inputs are finite; a program needn't handle non-finite values.
Results may differ from the reference program's by a relative error of at most 0.009.
Values are sent between devices in bfloat16 or wider.
A program may use at most 2 GiB of HBM per device.

```python
import jax
import jax.numpy as jnp

MEMBERS = 16
TOKENS = 256
D = 3584
FF = 2048
TOP = 8
EXPERTS = 48
SHARED_FF = 2048
SLOTS = 5 * TOKENS * TOP // (4 * EXPERTS)


def setup_inputs(seed: int = 0, part: int = 0) -> dict:
    own, k1, k2, k3, k4, k5, k6 = jax.random.split(jax.random.key(seed), 7)
    kx, ke, kl, kg = jax.random.split(jax.random.fold_in(own, part), 4)
    devices = (1, MEMBERS)
    place = jax.random.permutation(kl, jnp.arange(EXPERTS, dtype=jnp.uint32))
    slow = ((EXPERTS + (9 * place) % EXPERTS) << ((9 * place) // EXPERTS)) // EXPERTS
    wait = (jax.random.bits(ke, (*devices, TOKENS, EXPERTS), jnp.uint32) >> 10) * slow
    expert = jnp.argsort(wait, axis=-1)[..., :TOP].astype(jnp.int32)
    chosen = jax.nn.one_hot(expert, EXPERTS, dtype=jnp.int32)
    in_line = jnp.cumsum(chosen.reshape(*devices, TOKENS * TOP, EXPERTS), axis=2) - 1
    slot = jnp.sum(in_line.reshape(chosen.shape) * chosen, axis=-1)

    def one(key, rows, columns):
        return (jax.random.normal(key, (rows, columns), jnp.float32) * rows**-0.5).astype(jnp.bfloat16)

    def weights(key, rows, columns):
        return jax.lax.map(lambda k: one(k, rows, columns), jax.random.split(key, EXPERTS))

    return {
        "x": jax.random.normal(kx, (*devices, TOKENS, D), jnp.float32).astype(jnp.bfloat16),
        "expert": expert,
        "slot": slot,
        "gate": jax.nn.softmax(jax.random.normal(kg, expert.shape, jnp.float32)),
        "w_gate": weights(k1, D, FF),
        "w_up": weights(k2, D, FF),
        "w_down": weights(k3, FF, D),
        "s_gate": one(k4, D, SHARED_FF),
        "s_up": one(k5, D, SHARED_FF),
        "s_down": one(k6, SHARED_FF, D),
    }


def einsum(form, a, b):
    return jnp.einsum(form, a.astype(jnp.float32), b.astype(jnp.float32))


def for_all(x, s_gate, s_up, s_down):
    h = jax.nn.silu(einsum("...d,df->...f", x, s_gate)) * einsum("...d,df->...f", x, s_up)
    return einsum("...f,fd->...d", h.astype(jnp.bfloat16), s_down)


def reference(x, expert, slot, gate, w_gate, w_up, w_down, s_gate, s_up, s_down):
    to_expert = jax.nn.one_hot(expert, EXPERTS, dtype=jnp.bfloat16)
    to_slot = jax.nn.one_hot(slot, SLOTS, dtype=jnp.bfloat16)
    weighted = to_expert * gate[..., None].astype(jnp.bfloat16)
    dispatch = einsum("abtke,abtkc->abtec", to_expert, to_slot).astype(jnp.bfloat16)
    combine = einsum("abtke,abtkc->abtec", weighted, to_slot).astype(jnp.bfloat16)
    z = einsum("abtec,abtd->aebcd", dispatch, x).astype(jnp.bfloat16)
    h = jax.nn.silu(einsum("aebcd,edf->aebcf", z, w_gate))
    h = (h * einsum("aebcd,edf->aebcf", z, w_up)).astype(jnp.bfloat16)
    out = einsum("aebcf,efd->aebcd", h, w_down).astype(jnp.bfloat16)
    y = einsum("abtec,aebcd->abtd", combine, out)
    return (y + for_all(x, s_gate, s_up, s_down)).astype(jnp.bfloat16)
```

```python
import functools

import jax
import jax.numpy as jnp
from jax import lax
from jax.experimental import pallas as pl
from jax.experimental.pallas import tpu as pltpu
from jax.sharding import PartitionSpec as P

F32, BF16 = jnp.float32, jnp.bfloat16
CW = 512
PAD = 56
PARTS = ((0, 96, (8, 4, 2)), (96, 80, (4, 2, 8)), (176, 80, (2, 8, 4)))
VMEM_LIMIT = 67043328


def _dot(a, b):
    return lax.dot_general(a, b, (((1,), (0,)), ((), ())), preferred_element_type=F32)


def _place(axis):
    me = lax.axis_index(axis)
    bits = {8: me // 8, 4: (me // 4) % 2, 2: (me // 2) % 2, 1: me % 2}

    def flip(mask):
        d = me
        for b, v in bits.items():
            if mask & b:
                d = d + b * (1 - 2 * v)
        return d

    return me, bits, flip


def _greet(axis, others):
    barrier = pltpu.get_barrier_semaphore()
    for d in others:
        pl.semaphore_signal(barrier, inc=1, device_id={axis: d}, device_id_type=pl.DeviceIdType.MESH)
    pl.semaphore_wait(barrier, len(others))


def _wait(ref, sem):
    pltpu.make_async_copy(ref, ref, sem).wait()


def _up_kernel(
    axis, chunks, experts,
    x, meta, wg, wu, sg, su,
    xg, metag, h, hs,
    xv, xbuf, z, acc, wbuf, onehot, mv, stage,
    send_sem, phase_sem, pair_sem, meta_send, meta_recv, wsem, xsem, lsem, hsem,
):
    me, bits, flip = _place(axis)
    tokens, ff = x.shape[0], wg.shape[2]
    tiles = ff // 512

    def cols(n):
        return pl.ds(pl.multiple_of(n * CW, CW), CW)

    def remote(src, dst, send, recv, mask):
        pltpu.make_async_remote_copy(
            src_ref=src, dst_ref=dst, send_sem=send, recv_sem=recv,
            device_id={axis: flip(mask)}, device_id_type=pl.DeviceIdType.MESH,
        ).start()

    def send(block, n, i, to, phase):
        lo, size, _ = PARTS[i]
        d = flip(block)
        there = xg.at[d, pl.ds(lo, size), cols(n)]
        here = x.at[pl.ds(lo, size), cols(n)] if block == 0 else there
        recv = pair_sem.at[n] if to == 1 else phase_sem.at[n, i, phase]
        remote(here, there, send_sem, recv, to)

    def t0(n):
        for phase in range(3):
            for i, (_, _, dims) in enumerate(PARTS):
                send(0, n, i, dims[phase], phase)
        remote(x.at[:, cols(n)], xg.at[me, :, cols(n)], send_sem, pair_sem.at[n], 1)

    def arrived(n, i, phase, blocks):
        lo, size, _ = PARTS[i]
        _wait(xg.at[pl.ds(0, blocks), pl.ds(lo, size), cols(n)], phase_sem.at[n, i, phase])

    def t1(n):
        for i, (_, _, (a, b, c)) in enumerate(PARTS):
            arrived(n, i, 0, 1)
            send(a, n, i, b, 1)
            send(a, n, i, c, 2)
            send(a, n, i, 1, 0)

    def t2(n):
        for i, (_, _, (a, b, c)) in enumerate(PARTS):
            arrived(n, i, 1, 2)
            for block in (b, a + b):
                send(block, n, i, c, 2)
                send(block, n, i, 1, 0)

    def t3(n):
        for i, (_, _, (a, b, c)) in enumerate(PARTS):
            arrived(n, i, 2, 4)
            for block in (c, a + c, b + c, a + b + c):
                send(block, n, i, 1, 0)

    def t4(n):
        _wait(xg.at[pl.ds(0, 8), :, cols(n)], pair_sem.at[n])
        for block in range(16):
            d = flip(block)
            src = x.at[:, cols(n)] if block == 0 else xg.at[d, :, cols(n)]
            pltpu.make_async_copy(src, xbuf.at[d], xsem).start()

    def weights(n, e, slot):
        for half, w in enumerate((wg, wu)):
            pltpu.make_async_copy(w.at[e, cols(n), :], wbuf.at[slot, half], wsem.at[slot, half]).start()

    def shared_weights(k, slot):
        for half, w in enumerate((sg, su)):
            pltpu.make_async_copy(w.at[cols(k), :], wbuf.at[slot, half], wsem.at[slot, half]).start()

    def have(slot, half):
        _wait(wbuf.at[slot, half], wsem.at[slot, half])

    own = pltpu.make_async_copy(x, xv, lsem)
    own.start()
    shared_weights(0, 0)
    _greet(axis, [flip(m) for m in range(1, 16)])
    t0(0)
    for m in range(1, 16):
        d = flip(m)
        remote(meta.at[d], metag.at[me], meta_send, meta_recv, m)
    t0(1)
    acc[0, pl.ds(0, tokens), :] = jnp.zeros((tokens, 2 * ff), F32)
    own.wait()

    for k in range(chunks):
        slot = k % 2
        if k + 1 < chunks:
            shared_weights(k + 1, 1 - slot)
        else:
            weights(0, 0, 1 - slot)
        for half in range(2):
            have(slot, half)

            def tile(j, _):
                at = pl.ds(pl.multiple_of(half * ff + j * 512, 512), 512)
                w = wbuf[slot, half, :, pl.ds(pl.multiple_of(j * 512, 512), 512)]
                acc[0, pl.ds(0, tokens), at] += _dot(xv[:, k * CW:(k + 1) * CW], w)
                return 0

            lax.fori_loop(0, tiles, tile, 0)
        if k == 1:
            _wait(metag.at[pl.ds(0, 15)], meta_recv)
            for m in range(16):
                d = flip(m)
                pltpu.make_async_copy(meta.at[d] if m == 0 else metag.at[d], mv.at[d], lsem).start()
            t1(0)
        if k == 4:
            t2(0)

    def shared_h(j, _):
        g = acc[0, pl.ds(0, tokens), pl.ds(pl.multiple_of(j * 512, 512), 512)]
        u = acc[0, pl.ds(0, tokens), pl.ds(pl.multiple_of(ff + j * 512, 512), 512)]
        v = (g * jax.nn.sigmoid(g) * u).astype(BF16)
        xv[:, pl.ds(pl.multiple_of(j * 512, 512), 512)] = v
        return 0

    lax.fori_loop(0, tiles, shared_h, 0)
    hs_out = pltpu.make_async_copy(xv.at[:, pl.ds(0, ff)], hs, hsem.at[2])
    hs_out.start()

    _wait(mv, lsem)
    pltpu.make_async_copy(mv.at[me], metag.at[me], lsem).start()
    row = lax.broadcasted_iota(jnp.int32, (PAD, tokens), 0).astype(F32)

    def build(s, _):
        pos = mv[s].astype(F32)
        for e in range(experts):
            hit = jnp.where(pos[e:e + 1, :] == row, 1.0, 0.0)
            onehot[s, e] = hit.astype(BF16)
        return 0

    lax.fori_loop(0, 16, build, 0)
    t3(0)
    t4(0)

    def chunk(n, first, last):
        _wait(xbuf, xsem)

        def pair(p, _):
            got = []
            for i in range(2):
                s = 2 * p + i
                m = jnp.concatenate([onehot[s, e] for e in range(experts)], 0)
                got.append(_dot(m, xbuf[s]))
            for e in range(experts):
                both = jnp.concatenate([v[PAD * e:PAD * (e + 1)] for v in got], 0)
                z[e, pl.ds(pl.multiple_of(p * 2 * PAD, 16), 2 * PAD), :] = both.astype(BF16)
            return 0

        lax.fori_loop(0, 8, pair, 0)

        for e in range(experts):
            slot = (chunks + experts * n + e) % 2
            if e + 1 < experts:
                weights(n, e + 1, 1 - slot)
            elif not last:
                weights(n + 1, 0, 1 - slot)
            if last:
                have(slot, 0)
                have(slot, 1)

                def finish(j, _):
                    at = pl.ds(pl.multiple_of(j * 512, 512), 512)
                    at_u = pl.ds(pl.multiple_of(ff + j * 512, 512), 512)
                    side = j % 2

                    @pl.when(e * tiles + j >= 2)
                    def _():
                        _wait(stage.at[side], hsem.at[side])

                    def rows(i, _):
                        r = pl.ds(pl.multiple_of(i * 224, 224), 224)
                        g = acc[e, r, at] + _dot(z[e, r, :], wbuf[slot, 0, :, at])
                        u = acc[e, r, at_u] + _dot(z[e, r, :], wbuf[slot, 1, :, at])
                        stage[side, r, :] = (g * jax.nn.sigmoid(g) * u).astype(BF16)
                        return 0

                    lax.fori_loop(0, 16 * PAD // 224, rows, 0)
                    pltpu.make_async_copy(stage.at[side], h.at[e, :, at], hsem.at[side]).start()
                    return 0

                lax.fori_loop(0, tiles, finish, 0)
            else:
                for half in range(2):
                    have(slot, half)

                    def tile(j, _):
                        at = pl.ds(pl.multiple_of(half * ff + j * 512, 512), 512)
                        w = wbuf[slot, half, :, pl.ds(pl.multiple_of(j * 512, 512), 512)]
                        if first:
                            acc[e, :, at] = _dot(z[e], w)
                        else:
                            acc[e, :, at] += _dot(z[e], w)
                        return 0

                    lax.fori_loop(0, tiles, tile, 0)
                    point = 2 * e + half
                    if point == 0:
                        t1(n + 1)
                    if point == 2:
                        t2(n + 1)
                    if point == 3:
                        @pl.when(n + 2 < chunks)
                        def _():
                            t0(n + 2)
                    if point == 4:
                        t3(n + 1)
        if not last:
            t4(n + 1)

    chunk(0, True, False)

    def middle(n, _):
        chunk(n, False, False)
        return 0

    lax.fori_loop(1, chunks - 1, middle, 0)
    chunk(chunks - 1, False, True)
    for side in range(2):
        _wait(stage.at[side], hsem.at[side])
    hs_out.wait()
    _wait(mv.at[0], lsem)
    _wait(metag.at[pl.ds(0, 15)], meta_send)
    _wait(xg.at[pl.ds(0, 15)], send_sem)


def _down_kernel(
    axis, chunks, experts,
    h, hs, metag, wd, sd,
    y,
    hv, hsv, out32, wbuf, weight_t, mv, own, give, take, s1, s2, s3, r1, r2, r3, ost,
    hsem, lsem, wsem, give_sem, take_sem, credit, ss1, ss2, ss3, rs1, rs2, rs3, osem,
):
    me, bits, flip = _place(axis)
    tokens = hs.shape[0]

    def cols(n):
        return pl.ds(pl.multiple_of(n * CW, CW), CW)

    def remote(src, dst, send, recv, mask):
        pltpu.make_async_remote_copy(
            src_ref=src, dst_ref=dst, send_sem=send, recv_sem=recv,
            device_id={axis: flip(mask)}, device_id_type=pl.DeviceIdType.MESH,
        ).start()

    def weights(n, e, slot):
        src = wd.at[e, :, cols(n)] if e < experts else sd.at[:, cols(n)]
        pltpu.make_async_copy(src, wbuf.at[slot], wsem.at[slot]).start()

    for e in range(experts):
        pltpu.make_async_copy(h.at[e], hv.at[e], hsem.at[e]).start()
    weights(0, 0, 0)
    pltpu.make_async_copy(hs, hsv, hsem.at[experts]).start()
    copy = pltpu.make_async_copy(metag, mv, lsem)
    copy.start()
    _greet(axis, [flip(m) for m in (8, 4, 2, 1)])
    copy.wait()

    row = lax.broadcasted_iota(jnp.int32, (PAD, tokens), 0).astype(F32)
    rest = jnp.zeros((256 - experts * PAD, tokens), F32)

    def build(s, _):
        v = mv[s].astype(F32)
        hits = [jnp.where(v[e:e + 1, :] == row, v[experts + e:experts + e + 1, :], 0.0) for e in range(experts)]
        weight_t[s] = jnp.transpose(jnp.concatenate([*hits, rest], 0)).astype(BF16)
        return 0

    lax.fori_loop(0, 16, build, 0)

    def part(i):
        lo, size, dims = PARTS[i]
        return pl.ds(lo, size), dims

    def f32(ref, *at):
        return ref[at].astype(F32)

    def sum_at(n, block, r):
        p = n % 2
        return own[p, block // 2, r, :] + f32(take, p, block // 2, r, slice(None))

    def stage1(n):
        p = n % 2
        _wait(take.at[p], take_sem.at[p])

        @pl.when(n >= 2)
        def _():
            _wait(s1.at[p], ss1.at[p])

        for i in range(3):
            r, (a, b, c) = part(i)
            for k, q in enumerate((b + c, b, c, 0)):
                s1[p, k, r, :] = sum_at(n, q + a, r).astype(BF16)
                remote(s1.at[p, k, r], r1.at[n, k, r], ss1.at[p], rs1.at[n, i, k], a)

    def stage2(n):
        p = n % 2

        @pl.when(n >= 2)
        def _():
            _wait(s2.at[p], ss2.at[p])

        for i in range(3):
            r, (a, b, c) = part(i)
            for k, q in enumerate((b + c, b)):
                _wait(r1.at[n, k, r], rs1.at[n, i, k])
                v = sum_at(n, q, r) + f32(r1, n, k, r, slice(None))
                s2[p, k, r, :] = v.astype(BF16)
                remote(s2.at[p, k, r], r2.at[n, k, r], ss2.at[p], rs2.at[n, i, k], b)

    def stage3(n):
        p = n % 2

        @pl.when(n >= 2)
        def _():
            _wait(s3.at[p], ss3.at[p])

        for i in range(3):
            r, (a, b, c) = part(i)
            _wait(r1.at[n, 2, r], rs1.at[n, i, 2])
            _wait(r2.at[n, 0, r], rs2.at[n, i, 0])
            v = sum_at(n, c, r) + f32(r1, n, 2, r, slice(None)) + f32(r2, n, 0, r, slice(None))
            s3[p, r, :] = v.astype(BF16)
            remote(s3.at[p, r], r3.at[n, r], ss3.at[p], rs3.at[n, i], c)

    def stage4(n):
        p = n % 2

        @pl.when(n >= 2)
        def _():
            _wait(ost.at[p], osem.at[p])

        for i in range(3):
            r, (a, b, c) = part(i)
            _wait(r1.at[n, 3, r], rs1.at[n, i, 3])
            _wait(r2.at[n, 1, r], rs2.at[n, i, 1])
            _wait(r3.at[n, r], rs3.at[n, i])
            v = sum_at(n, 0, r) + f32(r1, n, 3, r, slice(None)) + f32(r2, n, 1, r, slice(None))
            ost[p, r, :] = (v + f32(r3, n, r, slice(None))).astype(BF16)
        pltpu.make_async_copy(ost.at[p], y.at[:, cols(n)], osem.at[p]).start()
        pl.semaphore_signal(credit, inc=1, device_id={axis: flip(1)}, device_id_type=pl.DeviceIdType.MESH)

    for e in range(experts + 1):
        _wait(hv.at[e] if e < experts else hsv, hsem.at[e])

    def combine(r, core):
        s = 8 * ((bits[8] + r // 4) % 2) + 4 * ((bits[4] + (r // 2) % 2) % 2) + 2 * ((bits[2] + r % 2) % 2) + core
        at = pl.ds(pl.multiple_of(s * PAD, 8), PAD)
        rest = jnp.zeros((256 - experts * PAD, CW), F32)
        v = jnp.concatenate([*(out32[e, at, :] for e in range(experts)), rest], 0).astype(BF16)
        return _dot(weight_t[s], v)

    def chunk(n, _):
        p = n % 2
        for e in range(experts):
            slot = e % 2
            weights(n, e + 1, 1 - slot)
            _wait(wbuf.at[slot], wsem.at[slot])
            out32[e] = _dot(hv[e], wbuf[slot])
            if e == 0:
                @pl.when(n >= 1)
                def _():
                    stage1(n - 1)
            if e == 1:
                @pl.when(n >= 2)
                def _():
                    stage3(n - 2)
            if e == 2:
                @pl.when(n >= 2)
                def _():
                    stage4(n - 2)

        @pl.when(n + 1 < chunks)
        def _():
            weights(n + 1, 0, 0)

        @pl.when(n >= 2)
        def _():
            _wait(give.at[p], give_sem.at[p])
            pl.semaphore_wait(credit, 1)

        def others(r, _):
            give[p, r] = combine(r, 1 - bits[1]).astype(BF16)
            remote(give.at[p, r], take.at[p, r], give_sem.at[p], take_sem.at[p], 1)
            return 0

        lax.fori_loop(0, 8, others, 0)

        @pl.when(n >= 1)
        def _():
            stage2(n - 1)

        def mine(r, _):
            own[p, r] = combine(r, bits[1])
            return 0

        lax.fori_loop(1, 8, mine, 0)
        _wait(wbuf.at[1], wsem.at[1])
        own[p, 0] = combine(0, bits[1]) + _dot(hsv[...], wbuf[1])
        return 0

    lax.fori_loop(0, chunks, chunk, 0)
    stage1(chunks - 1)
    stage3(chunks - 2)
    stage4(chunks - 2)
    stage2(chunks - 1)
    stage3(chunks - 1)
    stage4(chunks - 1)
    for p in range(2):
        _wait(give.at[p], give_sem.at[p])
        _wait(s1.at[p], ss1.at[p])
        _wait(s2.at[p], ss2.at[p])
        _wait(s3.at[p], ss3.at[p])
        _wait(ost.at[p], osem.at[p])
    pl.semaphore_wait(credit, 2)


def _table(expert, slot, gate, members, experts, slots):
    tokens, top = expert.shape
    hit = expert[None] == jnp.arange(members * experts, dtype=jnp.int32)[:, None, None]
    hit = hit & (slot < slots)[None]
    pos = jnp.sum(jnp.where(hit, slot[None] + 1, 0), axis=-1) - 1
    weight = jnp.sum(jnp.where(hit, gate.astype(BF16).astype(F32)[None], 0.0), axis=-1)
    pos = pos.astype(BF16).reshape(members, experts, tokens)
    weight = weight.astype(BF16).reshape(members, experts, tokens)
    rest = jnp.zeros((members, 16 - 2 * experts, tokens), BF16)
    return jnp.concatenate([pos, weight, rest], axis=1)


def solution(mesh):
    axis, members = "ep", mesh.shape["ep"]

    def local(x, expert, slot, gate, w_gate, w_up, w_down, s_gate, s_up, s_down):
        x, expert, slot, gate = x[0, 0], expert[0, 0], slot[0, 0], gate[0, 0]
        tokens, d = x.shape
        experts, _, ff = w_gate.shape
        slots = 5 * tokens * expert.shape[1] // (4 * experts * members)
        chunks, rows = d // CW, members * PAD
        meta = _table(expert, slot, gate, members, experts, slots)
        hbm, dma = pl.BlockSpec(memory_space=pl.ANY), pltpu.SemaphoreType.DMA
        _, metag, h, hs = pl.pallas_call(
            functools.partial(_up_kernel, axis, chunks, experts),
            name="gather_up",
            out_shape=(
                jax.ShapeDtypeStruct((members, tokens, d), BF16),
                jax.ShapeDtypeStruct(meta.shape, BF16),
                jax.ShapeDtypeStruct((experts, rows, ff), BF16),
                jax.ShapeDtypeStruct((tokens, ff), BF16),
            ),
            in_specs=[hbm] * 6,
            out_specs=(hbm,) * 4,
            scratch_shapes=[
                pltpu.VMEM((tokens, d), BF16),
                pltpu.VMEM((members, tokens, CW), BF16),
                pltpu.VMEM((experts, rows, CW), BF16),
                pltpu.VMEM((experts, rows, 2 * ff), F32),
                pltpu.VMEM((2, 2, CW, ff), BF16),
                pltpu.VMEM((members, experts, PAD, tokens), BF16),
                pltpu.VMEM(meta.shape, BF16),
                pltpu.VMEM((2, rows, 512), BF16),
                dma, dma((chunks, 3, 3)), dma((chunks,)), dma, dma, dma((2, 2)), dma, dma, dma((3,)),
            ],
            compiler_params=pltpu.CompilerParams(
                collective_id=0, has_side_effects=True, vmem_limit_bytes=VMEM_LIMIT
            ),
        )(x, meta, w_gate, w_up, s_gate, s_up)
        y = pl.pallas_call(
            functools.partial(_down_kernel, axis, chunks, experts),
            name="down_scatter",
            out_shape=jax.ShapeDtypeStruct((tokens, d), BF16),
            in_specs=[hbm] * 5,
            out_specs=hbm,
            scratch_shapes=[
                pltpu.VMEM((experts, rows, ff), BF16),
                pltpu.VMEM((tokens, ff), BF16),
                pltpu.VMEM((experts, rows, CW), F32),
                pltpu.VMEM((2, ff, CW), BF16),
                pltpu.VMEM((members, tokens, 256), BF16),
                pltpu.VMEM(meta.shape, BF16),
                pltpu.VMEM((2, 8, tokens, CW), F32),
                pltpu.VMEM((2, 8, tokens, CW), BF16),
                pltpu.VMEM((2, 8, tokens, CW), BF16),
                pltpu.VMEM((2, 4, tokens, CW), BF16),
                pltpu.VMEM((2, 2, tokens, CW), BF16),
                pltpu.VMEM((2, tokens, CW), BF16),
                pltpu.VMEM((chunks, 4, tokens, CW), BF16),
                pltpu.VMEM((chunks, 2, tokens, CW), BF16),
                pltpu.VMEM((chunks, tokens, CW), BF16),
                pltpu.VMEM((2, tokens, CW), BF16),
                dma((experts + 1,)), dma, dma((2,)), dma((2,)), dma((2,)), pltpu.SemaphoreType.REGULAR,
                dma((2,)), dma((2,)), dma((2,)),
                dma((chunks, 3, 4)), dma((chunks, 3, 2)), dma((chunks, 3)), dma((2,)),
            ],
            compiler_params=pltpu.CompilerParams(
                collective_id=1, has_side_effects=True, vmem_limit_bytes=VMEM_LIMIT
            ),
        )(h, hs, metag, w_down, s_down)
        return y[None, None]

    tok = P("dp", "ep", None, None)
    own = P("ep", None, None)
    return jax.shard_map(
        local,
        mesh=mesh,
        in_specs=(tok, tok, tok, tok, own, own, own, P(), P(), P()),
        out_specs=tok,
        check_vma=False,
    )
```

```python
import functools

import jax
import jax.numpy as jnp
from jax import lax
from jax.experimental import pallas as pl
from jax.experimental.pallas import tpu as pltpu
from jax.sharding import PartitionSpec as P

F32, BF16 = jnp.float32, jnp.bfloat16
CW = 512
CB = 512
WIN = 64
NONE = -1024.0
LAG = 3
PARTS = ((0, 96, (8, 4, 2)), (96, 80, (4, 2, 8)), (176, 80, (2, 8, 4)))
VMEM_LIMIT = 67043328


def _dot(a, b):
    return lax.dot_general(a, b, (((1,), (0,)), ((), ())), preferred_element_type=F32)


def _place(axis):
    me = lax.axis_index(axis)
    bits = {8: me // 8, 4: (me // 4) % 2, 2: (me // 2) % 2, 1: me % 2}

    def flip(mask):
        d = me
        for b, v in bits.items():
            if mask & b:
                d = d + b * (1 - 2 * v)
        return d

    return me, bits, flip


def _greet(axis, others):
    barrier = pltpu.get_barrier_semaphore()
    for d in others:
        pl.semaphore_signal(barrier, inc=1, device_id={axis: d}, device_id_type=pl.DeviceIdType.MESH)
    pl.semaphore_wait(barrier, len(others))


def _wait(ref, sem):
    pltpu.make_async_copy(ref, ref, sem).wait()


def _up_kernel(
    axis, chunks, experts, slots,
    x, expert, slot, gate, wg, wu, sg, su,
    xg, metag, h, hs,
    xbuf, z, acc, wbuf, onehot, ev, sv, gv, mt, mv,
    send_sem, phase_sem, pair_sem, meta_send, meta_recv, wsem, xsem, lsem, rsem, hsem,
):
    me, bits, flip = _place(axis)
    tokens, ff = x.shape[0], wg.shape[2]
    rows = 16 * slots

    def cols(n):
        return pl.ds(pl.multiple_of(n * CW, CW), CW)

    def remote(src, dst, send, recv, mask):
        pltpu.make_async_remote_copy(
            src_ref=src, dst_ref=dst, send_sem=send, recv_sem=recv,
            device_id={axis: flip(mask)}, device_id_type=pl.DeviceIdType.MESH,
        ).start()

    def send(block, n, i, to, phase):
        lo, size, _ = PARTS[i]
        d = flip(block)
        there = xg.at[d, pl.ds(lo, size), cols(n)]
        here = x.at[pl.ds(lo, size), cols(n)] if block == 0 else there
        recv = pair_sem.at[n] if to == 1 else phase_sem.at[n, i, phase]
        remote(here, there, send_sem, recv, to)

    def t0(n, *phases):
        for phase in phases:
            for i, (_, _, dims) in enumerate(PARTS):
                send(0, n, i, dims[phase], phase)
        if 2 in phases:
            remote(x.at[:, cols(n)], xg.at[me, :, cols(n)], send_sem, pair_sem.at[n], 1)

    def arrived(n, i, phase, blocks):
        lo, size, _ = PARTS[i]
        _wait(xg.at[pl.ds(0, blocks), pl.ds(lo, size), cols(n)], phase_sem.at[n, i, phase])

    def t1(n):
        for i, (_, _, (a, b, c)) in enumerate(PARTS):
            arrived(n, i, 0, 1)
            send(a, n, i, b, 1)
            send(a, n, i, c, 2)
            send(a, n, i, 1, 0)

    def t2(n):
        for i, (_, _, (a, b, c)) in enumerate(PARTS):
            arrived(n, i, 1, 2)
            for block in (b, a + b):
                send(block, n, i, c, 2)
                send(block, n, i, 1, 0)

    def t3(n):
        for i, (_, _, (a, b, c)) in enumerate(PARTS):
            arrived(n, i, 2, 4)
            for block in (c, a + c, b + c, a + b + c):
                send(block, n, i, 1, 0)

    def block_rows(s):
        return pl.ds(pl.multiple_of(s * tokens, tokens), tokens)

    def t4(n):
        _wait(xg.at[pl.ds(0, 8), :, cols(n)], pair_sem.at[n])
        for block in range(16):
            d = flip(block)
            src = x.at[:, cols(n)] if block == 0 else xg.at[d, :, cols(n)]
            pltpu.make_async_copy(src, xbuf.at[block_rows(d)], xsem).start()

    def weights(n, e, side):
        for half, w in enumerate((wg, wu)):
            pltpu.make_async_copy(w.at[e, cols(n), :], wbuf.at[side, half], wsem.at[side, half]).start()

    def shared_weights(k, side):
        for half, w in enumerate((sg, su)):
            pltpu.make_async_copy(w.at[cols(k), :], wbuf.at[side, half], wsem.at[side, half]).start()

    def have(side, half):
        _wait(wbuf.at[side, half], wsem.at[side, half])

    for k in range(chunks):
        pltpu.make_async_copy(x.at[:, cols(k)], xbuf.at[block_rows(k)], lsem).start()
    routing = [pltpu.make_async_copy(a, b, rsem.at[i]) for i, (a, b) in enumerate(((expert, ev), (slot, sv), (gate, gv)))]
    for copy in routing:
        copy.start()
    shared_weights(0, 0)
    _greet(axis, [flip(m) for m in range(1, 16)])
    t0(0, 0, 1, 2)

    for copy in routing:
        copy.wait()

    et, st, gt = ev[...].astype(F32), sv[...].astype(F32), gv[...].astype(BF16).astype(F32)
    kept = st < slots

    def table(d, _):
        pos, weight = [], []
        for j in range(experts):
            hit = (et == (experts * d + j).astype(F32)) & kept
            pos.append(jnp.sum(jnp.where(hit, st - NONE, 0.0), axis=0, keepdims=True) + NONE)
            weight.append(jnp.sum(jnp.where(hit, gt, 0.0), axis=0, keepdims=True))
        rest = jnp.zeros((16 - 2 * experts, tokens), F32)
        mt[d] = jnp.concatenate([*pos, *weight, rest], 0).astype(BF16)
        return 0

    lax.fori_loop(0, 16, table, 0)
    for m in range(1, 16):
        remote(mt.at[flip(m)], mv.at[me], meta_send, meta_recv, m)
    mv[me] = mt[me]
    acc[0, pl.ds(0, tokens), :] = jnp.zeros((tokens, 2 * ff), F32)
    _wait(xbuf.at[pl.ds(0, chunks * tokens)], lsem)

    for k in range(chunks):
        side = k % 2
        if k + 1 < chunks:
            shared_weights(k + 1, 1 - side)
        else:
            weights(0, 0, 1 - side)
        for half in range(2):
            have(side, half)
            acc[0, pl.ds(0, tokens), pl.ds(half * ff, ff)] += _dot(xbuf[pl.ds(k * tokens, tokens), :], wbuf[side, half])
        if k == 1:
            t1(0)
        if k == 4:
            t2(0)
            t0(1, 0, 1, 2)

    def shared_h(j, _):
        g = acc[0, pl.ds(0, tokens), pl.ds(pl.multiple_of(j * 512, 512), 512)]
        u = acc[0, pl.ds(0, tokens), pl.ds(pl.multiple_of(ff + j * 512, 512), 512)]
        there = block_rows(chunks + j)
        xbuf[there, :] = (g * jax.nn.sigmoid(g) * u).astype(BF16)
        pltpu.make_async_copy(xbuf.at[there], hs.at[:, pl.ds(pl.multiple_of(j * 512, 512), 512)], lsem).start()
        return 0

    lax.fori_loop(0, ff // 512, shared_h, 0)

    _wait(mv.at[pl.ds(0, 15)], meta_recv)
    meta_out = pltpu.make_async_copy(mv, metag, rsem.at[0])
    meta_out.start()
    row = lax.broadcasted_iota(jnp.int32, (WIN, tokens), 0).astype(F32)

    def build(s, _):
        pos = mv[s].astype(F32) + ((s * slots) % 8).astype(F32)
        for e in range(experts):
            onehot[s, pl.ds(e * WIN, WIN), :] = jnp.where(pos[e:e + 1, :] == row, 1.0, 0.0).astype(BF16)
        return 0

    lax.fori_loop(0, 16, build, 0)
    t3(0)

    def clear(i, _):
        e, part = i // (ff // 256), i % (ff // 256)
        acc[e, :, pl.ds(pl.multiple_of(part * 512, 512), 512)] = jnp.zeros((rows, 512), F32)
        return 0

    lax.fori_loop(0, experts * 2 * ff // 512, clear, 0)
    _wait(xbuf.at[pl.ds(chunks * tokens, ff // 512 * tokens)], lsem)
    t4(0)
    t1(1)
    t0(2, 0, 1)

    def spread():
        held = [None] * experts
        over = [None] * experts
        done = [0] * experts
        for s in range(16):
            d = _dot(onehot[s], xbuf[pl.ds(s * tokens, tokens), :])
            size = 8 * ((s + 1) * slots // 8 - s * slots // 8)
            for e in range(experts):
                w = d[WIN * e:WIN * (e + 1)]
                v = [w[:size]] if over[e] is None else [w[:8] + over[e], w[8:size]]
                over[e] = w[size:size + 8] if (s + 1) * slots % 8 else None
                if held[e] is not None:
                    v = [held[e], *v]
                v = jnp.concatenate(v, 0) if len(v) > 1 else v[0]
                k = v.shape[0] // 16 * 16
                z[e, pl.ds(done[e], k), :] = v[:k].astype(BF16)
                held[e] = v[k:] if k < v.shape[0] else None
                done[e] += k

    def chunk(n, last):
        _wait(xbuf, xsem)
        spread()
        for e in range(experts):
            side = (chunks + experts * n + e) % 2
            if e + 1 < experts:
                weights(n, e + 1, 1 - side)
            elif not last:
                weights(n + 1, 0, 1 - side)
            if last:
                have(side, 0)
                have(side, 1)
                half_rows = rows // 32 * 16 + 16

                def finish(j, _):
                    at = pl.ds(pl.multiple_of(512 * j, 512), 512)
                    at_u = pl.ds(pl.multiple_of(ff + 512 * j, 512), 512)
                    there = pl.ds(pl.multiple_of(j * rows, 16), rows)
                    if e > 0:
                        _wait(xbuf.at[there], hsem.at[j])
                    for lo, size in ((0, half_rows), (half_rows, rows - half_rows)):
                        r = pl.ds(lo, size)
                        g = acc[e, r, at] + _dot(z[e, r, :], wbuf[side, 0, :, at])
                        u = acc[e, r, at_u] + _dot(z[e, r, :], wbuf[side, 1, :, at])
                        v = (g * jax.nn.sigmoid(g) * u).astype(BF16)
                        xbuf[pl.ds(pl.multiple_of(j * rows + lo, 16), size), :] = v
                    pltpu.make_async_copy(xbuf.at[there], h.at[e, :, at], hsem.at[j]).start()
                    return 0

                lax.fori_loop(0, ff // 512, finish, 0)
            else:
                for half in range(2):
                    have(side, half)
                    at = pl.ds(half * ff, ff)
                    acc[e, :, at] += _dot(z[e], wbuf[side, half])
                    point = 2 * e + half
                    if point == 0:
                        t2(n + 1)

                        @pl.when(n + 2 < chunks)
                        def _():
                            t0(n + 2, 2)
                    if point == 2:
                        @pl.when(n + 2 < chunks)
                        def _():
                            t1(n + 2)

                        @pl.when(n + 3 < chunks)
                        def _():
                            t0(n + 3, 0, 1)
                    if point == 3:
                        t3(n + 1)
                    if point == 4:
                        t4(n + 1)

    def most(n, _):
        chunk(n, False)
        return 0

    lax.fori_loop(0, chunks - 1, most, 0)
    chunk(chunks - 1, True)
    for k in range(ff // 512):
        _wait(xbuf.at[pl.ds(k * rows, rows)], hsem.at[k])
    meta_out.wait()
    _wait(mv.at[pl.ds(0, 15)], meta_send)
    _wait(xg.at[pl.ds(0, 15)], send_sem)


def _down_kernel(
    axis, chunks, experts, slots,
    h, hs, metag, wd, sd,
    y,
    hv, hsv, out32, wbuf, weight_t, mv, own, give, take, s1, s2, s3, r1, r2, r3, ost,
    hsem, lsem, wsem, give_sem, take_sem, credit, ss1, ss2, ss3, rs1, rs2, rs3, osem,
):
    me, bits, flip = _place(axis)
    tokens, rows = hs.shape[0], 16 * slots

    def cols(n):
        return pl.ds(pl.multiple_of(n * CB, CB), CB)

    def remote(src, dst, send, recv, mask):
        pltpu.make_async_remote_copy(
            src_ref=src, dst_ref=dst, send_sem=send, recv_sem=recv,
            device_id={axis: flip(mask)}, device_id_type=pl.DeviceIdType.MESH,
        ).start()

    def weights(n, e, side):
        src = wd.at[e, :, cols(n)] if e < experts else sd.at[:, cols(n)]
        pltpu.make_async_copy(src, wbuf.at[side], wsem.at[side]).start()

    copy = pltpu.make_async_copy(metag, mv, lsem)
    copy.start()
    pltpu.make_async_copy(h.at[0], hv.at[0], hsem.at[0]).start()
    weights(0, 0, 0)
    for e in range(1, experts):
        pltpu.make_async_copy(h.at[e], hv.at[e], hsem.at[e]).start()
    pltpu.make_async_copy(hs, hsv, hsem.at[experts]).start()
    _greet(axis, [flip(m) for m in (8, 4, 2, 1)])
    copy.wait()

    row = lax.broadcasted_iota(jnp.int32, (WIN, tokens), 0).astype(F32)
    rest = jnp.zeros((256 - experts * WIN, tokens), F32)

    def build(s, _):
        v = mv[s].astype(F32)
        shift = ((s * slots) % 8).astype(F32)
        hits = [
            jnp.where(v[e:e + 1, :] + shift == row, v[experts + e:experts + e + 1, :], 0.0) for e in range(experts)
        ]
        weight_t[s] = jnp.transpose(jnp.concatenate([*hits, rest], 0)).astype(BF16)
        return 0

    lax.fori_loop(0, 16, build, 0)
    for e in range(experts):
        out32[e, pl.ds(rows, 8), :] = jnp.zeros((8, CB), F32)

    def part(i):
        lo, size, dims = PARTS[i]
        return pl.ds(lo, size), dims

    def f32(ref, *at):
        return ref[at].astype(F32)

    def sum_at(n, block, r):
        p = n % LAG
        return own[p, block // 2, r, :] + f32(take, p, block // 2, r, slice(None))

    def free(n, ref, sem):
        @pl.when(n >= 2)
        def _():
            _wait(ref.at[n % 2], sem.at[n % 2])

    def stage1(n):
        p = n % 2
        _wait(take.at[n % LAG], take_sem.at[n % LAG])
        free(n, s1, ss1)
        for i in range(3):
            r, (a, b, c) = part(i)
            for k, q in enumerate((b + c, b, c, 0)):
                s1[p, k, r, :] = sum_at(n, q + a, r).astype(BF16)
                remote(s1.at[p, k, r], r1.at[n, k, r], ss1.at[p], rs1.at[n, i, k], a)

    def stage2(n):
        p = n % 2
        free(n, s2, ss2)
        for i in range(3):
            r, (a, b, c) = part(i)
            for k, q in enumerate((b + c, b)):
                _wait(r1.at[n, k, r], rs1.at[n, i, k])
                v = sum_at(n, q, r) + f32(r1, n, k, r, slice(None))
                s2[p, k, r, :] = v.astype(BF16)
                remote(s2.at[p, k, r], r2.at[n, k, r], ss2.at[p], rs2.at[n, i, k], b)

    def stage3(n):
        p = n % 2
        free(n, s3, ss3)
        for i in range(3):
            r, (a, b, c) = part(i)
            _wait(r1.at[n, 2, r], rs1.at[n, i, 2])
            _wait(r2.at[n, 0, r], rs2.at[n, i, 0])
            v = sum_at(n, c, r) + f32(r1, n, 2, r, slice(None)) + f32(r2, n, 0, r, slice(None))
            s3[p, r, :] = v.astype(BF16)
            remote(s3.at[p, r], r3.at[n, r], ss3.at[p], rs3.at[n, i], c)

    def stage4(n):
        p = n % 2
        free(n, ost, osem)
        for i in range(3):
            r, (a, b, c) = part(i)
            _wait(r1.at[n, 3, r], rs1.at[n, i, 3])
            _wait(r2.at[n, 1, r], rs2.at[n, i, 1])
            _wait(r3.at[n, r], rs3.at[n, i])
            v = sum_at(n, 0, r) + f32(r1, n, 3, r, slice(None)) + f32(r2, n, 1, r, slice(None))
            ost[p, r, :] = (v + f32(r3, n, r, slice(None))).astype(BF16)
        pltpu.make_async_copy(ost.at[p], y.at[:, cols(n)], osem.at[p]).start()
        pl.semaphore_signal(credit, inc=1, device_id={axis: flip(1)}, device_id_type=pl.DeviceIdType.MESH)

    def combine(r, core):
        s = flip(2 * r) - bits[1] + core
        at = pl.ds(pl.multiple_of(8 * ((s * slots) // 8), 8), WIN)
        rest = jnp.zeros((256 - experts * WIN, CB), F32)
        v = jnp.concatenate([*(out32[e, at, :] for e in range(experts)), rest], 0).astype(BF16)
        return _dot(weight_t[s], v)

    def late(n, k, stage):
        @pl.when((n >= k) & (n < chunks + k))
        def _():
            stage(n - k)

    def down(n, e):
        side = e % 2
        weights(n, e + 1, 1 - side)

        @pl.when(n == 0)
        def _():
            _wait(hv.at[e], hsem.at[e])

        _wait(wbuf.at[side], wsem.at[side])
        out32[e, pl.ds(0, rows), :] = _dot(hv[e], wbuf[side])

    def chunk(n, _):
        for e in range(experts):
            @pl.when(n < chunks)
            def _():
                down(n, e)

            if e == 0:
                late(n, 3, stage3)
                late(n, 1, stage1)
            if e == 1:
                late(n, 2, stage2)
            if e == 2:
                late(n, 3, stage4)

        @pl.when(n < chunks)
        def _():
            join(n)

        return 0

    def join(n):
        p = n % LAG

        @pl.when(n + 1 < chunks)
        def _():
            weights(n + 1, 0, 0)

        @pl.when(n >= 2)
        def _():
            _wait(give.at[n % 2], give_sem.at[n % 2])

        for r in range(8):
            give[n % 2, r] = combine(r, 1 - bits[1]).astype(BF16)

        @pl.when(n >= LAG)
        def _():
            pl.semaphore_wait(credit, 1)

        remote(give.at[n % 2], take.at[p], give_sem.at[n % 2], take_sem.at[p], 1)

        @pl.when(n == 0)
        def _():
            _wait(hsv, hsem.at[experts])

        _wait(wbuf.at[1], wsem.at[1])
        own[p, 0] = combine(0, bits[1]) + _dot(hsv[...], wbuf[1])
        for r in range(1, 8):
            own[p, r] = combine(r, bits[1])

    lax.fori_loop(0, chunks + LAG, chunk, 0)
    for p in range(2):
        _wait(give.at[p], give_sem.at[p])
        _wait(s1.at[p], ss1.at[p])
        _wait(s2.at[p], ss2.at[p])
        _wait(s3.at[p], ss3.at[p])
        _wait(ost.at[p], osem.at[p])
    pl.semaphore_wait(credit, LAG)


def solution(mesh):
    axis, members = "ep", mesh.shape["ep"]

    def local(x, expert, slot, gate, w_gate, w_up, w_down, s_gate, s_up, s_down):
        x, expert, slot, gate = x[0, 0], expert[0, 0], slot[0, 0], gate[0, 0]
        tokens, d = x.shape
        expert, slot, gate = expert.T, slot.T, gate.T
        experts, _, ff = w_gate.shape
        slots = 5 * tokens * expert.shape[0] // (4 * experts * members)
        rows = members * slots
        hbm, dma, vmem = pl.BlockSpec(memory_space=pl.ANY), pltpu.SemaphoreType.DMA, pltpu.VMEM
        table, chunks = (members, 16, tokens), d // CW
        _, metag, h, hs = pl.pallas_call(
            functools.partial(_up_kernel, axis, chunks, experts, slots),
            name="gather_up",
            out_shape=(
                jax.ShapeDtypeStruct((members, tokens, d), BF16),
                jax.ShapeDtypeStruct(table, BF16),
                jax.ShapeDtypeStruct((experts, rows, ff), BF16),
                jax.ShapeDtypeStruct((tokens, ff), BF16),
            ),
            in_specs=[hbm] * 8,
            out_specs=(hbm,) * 4,
            scratch_shapes=[
                vmem((members * tokens, CW), BF16),
                vmem((experts, rows, CW), BF16),
                vmem((experts, rows, 2 * ff), F32),
                vmem((2, 2, CW, ff), BF16),
                vmem((members, experts * WIN, tokens), BF16),
                vmem(expert.shape, jnp.int32),
                vmem(slot.shape, jnp.int32),
                vmem(gate.shape, F32),
                vmem(table, BF16),
                vmem(table, BF16),
                dma, dma((chunks, 3, 3)), dma((chunks,)), dma, dma, dma((2, 2)), dma, dma, dma((3,)), dma((ff // 512,)),
            ],
            compiler_params=pltpu.CompilerParams(
                collective_id=0, has_side_effects=True, vmem_limit_bytes=VMEM_LIMIT
            ),
        )(x, expert, slot, gate, w_gate, w_up, s_gate, s_up)
        chunks = d // CB
        y = pl.pallas_call(
            functools.partial(_down_kernel, axis, chunks, experts, slots),
            name="down_scatter",
            out_shape=jax.ShapeDtypeStruct((tokens, d), BF16),
            in_specs=[hbm] * 5,
            out_specs=hbm,
            scratch_shapes=[
                vmem((experts, rows, ff), BF16),
                vmem((tokens, ff), BF16),
                vmem((experts, rows + 8, CB), F32),
                vmem((2, ff, CB), BF16),
                vmem((members, tokens, 256), BF16),
                vmem(table, BF16),
                vmem((LAG, 8, tokens, CB), F32),
                vmem((2, 8, tokens, CB), BF16),
                vmem((LAG, 8, tokens, CB), BF16),
                vmem((2, 4, tokens, CB), BF16),
                vmem((2, 2, tokens, CB), BF16),
                vmem((2, tokens, CB), BF16),
                vmem((chunks, 4, tokens, CB), BF16),
                vmem((chunks, 2, tokens, CB), BF16),
                vmem((chunks, tokens, CB), BF16),
                vmem((2, tokens, CB), BF16),
                dma((experts + 1,)), dma, dma((2,)), dma((2,)), dma((LAG,)), pltpu.SemaphoreType.REGULAR,
                dma((2,)), dma((2,)), dma((2,)),
                dma((chunks, 3, 4)), dma((chunks, 3, 2)), dma((chunks, 3)), dma((2,)),
            ],
            compiler_params=pltpu.CompilerParams(
                collective_id=1, has_side_effects=True, vmem_limit_bytes=VMEM_LIMIT
            ),
        )(h, hs, metag, w_down, s_down)
        return y[None, None]

    tok = P("dp", "ep", None, None)
    own = P("ep", None, None)
    return jax.shard_map(
        local,
        mesh=mesh,
        in_specs=(tok, tok, tok, tok, own, own, own, P(), P(), P()),
        out_specs=tok,
        check_vma=False,
    )
```

```python
import functools

import jax
import jax.numpy as jnp
from jax import lax
from jax.experimental import pallas as pl
from jax.experimental.pallas import tpu as pltpu
from jax.sharding import PartitionSpec as P

F32, BF16 = jnp.float32, jnp.bfloat16
CW = 512
CB = 512
WIN = 64
NONE = -1024.0
LAG = 3
PARTS = ((0, 96, (8, 4, 2)), (96, 80, (4, 2, 8)), (176, 80, (2, 8, 4)))
VMEM_LIMIT = 67043328


def _dot(a, b):
    return lax.dot_general(a, b, (((1,), (0,)), ((), ())), preferred_element_type=F32)


def _place(axis):
    me = lax.axis_index(axis)
    bits = {8: me // 8, 4: (me // 4) % 2, 2: (me // 2) % 2, 1: me % 2}

    def flip(mask):
        d = me
        for b, v in bits.items():
            if mask & b:
                d = d + b * (1 - 2 * v)
        return d

    return me, bits, flip


def _greet(axis, others):
    barrier = pltpu.get_barrier_semaphore()
    for d in others:
        pl.semaphore_signal(barrier, inc=1, device_id={axis: d}, device_id_type=pl.DeviceIdType.MESH)
    pl.semaphore_wait(barrier, len(others))


def _wait(ref, sem):
    pltpu.make_async_copy(ref, ref, sem).wait()


def _up_kernel(
    axis, chunks, experts, slots,
    x, expert, slot, gate, wg, wu, sg, su,
    xg, metag, h, hs,
    xbuf, z, acc, wbuf, onehot, ev, sv, gv, mt, mv,
    send_sem, phase_sem, pair_sem, meta_send, meta_recv, wsem, xsem, lsem, rsem, hsem,
):
    me, bits, flip = _place(axis)
    tokens, ff = x.shape[0], wg.shape[2]
    rows = 16 * slots

    def cols(n):
        return pl.ds(pl.multiple_of(n * CW, CW), CW)

    def remote(src, dst, send, recv, mask):
        pltpu.make_async_remote_copy(
            src_ref=src, dst_ref=dst, send_sem=send, recv_sem=recv,
            device_id={axis: flip(mask)}, device_id_type=pl.DeviceIdType.MESH,
        ).start()

    def send(block, n, i, to, phase):
        lo, size, _ = PARTS[i]
        d = flip(block)
        there = xg.at[d, pl.ds(lo, size), cols(n)]
        here = x.at[pl.ds(lo, size), cols(n)] if block == 0 else there
        recv = pair_sem.at[n] if to == 1 else phase_sem.at[n, i, phase]
        remote(here, there, send_sem, recv, to)

    def t0(n, *phases):
        for phase in phases:
            for i, (_, _, dims) in enumerate(PARTS):
                send(0, n, i, dims[phase], phase)
        if 2 in phases:
            remote(x.at[:, cols(n)], xg.at[me, :, cols(n)], send_sem, pair_sem.at[n], 1)

    def arrived(n, i, phase, blocks):
        lo, size, _ = PARTS[i]
        _wait(xg.at[pl.ds(0, blocks), pl.ds(lo, size), cols(n)], phase_sem.at[n, i, phase])

    def t1(n):
        for i, (_, _, (a, b, c)) in enumerate(PARTS):
            arrived(n, i, 0, 1)
            send(a, n, i, b, 1)
            send(a, n, i, c, 2)
            send(a, n, i, 1, 0)

    def t2(n):
        for i, (_, _, (a, b, c)) in enumerate(PARTS):
            arrived(n, i, 1, 2)
            for block in (b, a + b):
                send(block, n, i, c, 2)
                send(block, n, i, 1, 0)

    def t3(n):
        for i, (_, _, (a, b, c)) in enumerate(PARTS):
            arrived(n, i, 2, 4)
            for block in (c, a + c, b + c, a + b + c):
                send(block, n, i, 1, 0)

    def block_rows(s):
        return pl.ds(pl.multiple_of(s * tokens, tokens), tokens)

    def t4(n):
        _wait(xg.at[pl.ds(0, 8), :, cols(n)], pair_sem.at[n])
        for block in range(16):
            d = flip(block)
            src = x.at[:, cols(n)] if block == 0 else xg.at[d, :, cols(n)]
            pltpu.make_async_copy(src, xbuf.at[block_rows(d)], xsem).start()

    def weights(n, e, side):
        for half, w in enumerate((wg, wu)):
            pltpu.make_async_copy(w.at[e, cols(n), :], wbuf.at[side, half], wsem.at[side, half]).start()

    def shared_weights(k, side):
        for half, w in enumerate((sg, su)):
            pltpu.make_async_copy(w.at[cols(k), :], wbuf.at[side, half], wsem.at[side, half]).start()

    def have(side, half):
        _wait(wbuf.at[side, half], wsem.at[side, half])

    for k in range(chunks):
        pltpu.make_async_copy(x.at[:, cols(k)], xbuf.at[block_rows(k)], lsem).start()
    routing = [pltpu.make_async_copy(a, b, rsem.at[i]) for i, (a, b) in enumerate(((expert, ev), (slot, sv), (gate, gv)))]
    for copy in routing:
        copy.start()
    shared_weights(0, 0)
    _greet(axis, [flip(m) for m in range(1, 16)])
    t0(0, 0, 1, 2)

    for copy in routing:
        copy.wait()

    et, st, gt = ev[...].astype(F32), sv[...].astype(F32), gv[...].astype(BF16).astype(F32)
    kept = st < slots

    def table(d, _):
        pos, weight = [], []
        for j in range(experts):
            hit = (et == (experts * d + j).astype(F32)) & kept
            pos.append(jnp.sum(jnp.where(hit, st - NONE, 0.0), axis=0, keepdims=True) + NONE)
            weight.append(jnp.sum(jnp.where(hit, gt, 0.0), axis=0, keepdims=True))
        rest = jnp.zeros((16 - 2 * experts, tokens), F32)
        mt[d] = jnp.concatenate([*pos, *weight, rest], 0).astype(BF16)
        return 0

    lax.fori_loop(0, 16, table, 0)
    for m in range(1, 16):
        remote(mt.at[flip(m)], mv.at[me], meta_send, meta_recv, m)
    mv[me] = mt[me]
    acc[0, pl.ds(0, tokens), :] = jnp.zeros((tokens, 2 * ff), F32)
    _wait(xbuf.at[pl.ds(0, chunks * tokens)], lsem)

    for k in range(chunks):
        side = k % 2
        if k + 1 < chunks:
            shared_weights(k + 1, 1 - side)
        else:
            weights(0, 0, 1 - side)
        for half in range(2):
            have(side, half)
            acc[0, pl.ds(0, tokens), pl.ds(half * ff, ff)] += _dot(xbuf[pl.ds(k * tokens, tokens), :], wbuf[side, half])
        if k == 1:
            t1(0)
        if k == 4:
            t2(0)
            t0(1, 0, 1, 2)

    def shared_h(j, _):
        g = acc[0, pl.ds(0, tokens), pl.ds(pl.multiple_of(j * 512, 512), 512)]
        u = acc[0, pl.ds(0, tokens), pl.ds(pl.multiple_of(ff + j * 512, 512), 512)]
        there = block_rows(chunks + j)
        xbuf[there, :] = (g * jax.nn.sigmoid(g) * u).astype(BF16)
        pltpu.make_async_copy(xbuf.at[there], hs.at[:, pl.ds(pl.multiple_of(j * 512, 512), 512)], lsem).start()
        return 0

    lax.fori_loop(0, ff // 512, shared_h, 0)

    _wait(mv.at[pl.ds(0, 15)], meta_recv)
    meta_out = pltpu.make_async_copy(mv, metag, rsem.at[0])
    meta_out.start()
    row = lax.broadcasted_iota(jnp.int32, (WIN, tokens), 0).astype(F32)

    def build(s, _):
        pos = mv[s].astype(F32) + ((s * slots) % 8).astype(F32)
        for e in range(experts):
            onehot[s, pl.ds(e * WIN, WIN), :] = jnp.where(pos[e:e + 1, :] == row, 1.0, 0.0).astype(BF16)
        return 0

    lax.fori_loop(0, 16, build, 0)
    def clear(i, _):
        e, part = i // (ff // 256), i % (ff // 256)
        acc[e, :, pl.ds(pl.multiple_of(part * 512, 512), 512)] = jnp.zeros((rows, 512), F32)
        return 0

    lax.fori_loop(0, experts * 2 * ff // 512, clear, 0)
    t3(0)
    _wait(xbuf.at[pl.ds(chunks * tokens, ff // 512 * tokens)], lsem)
    t4(0)
    t1(1)
    t0(2, 0, 1)

    def spread():
        held = [None] * experts
        over = [None] * experts
        done = [0] * experts
        for s in range(16):
            d = _dot(onehot[s], xbuf[pl.ds(s * tokens, tokens), :])
            size = 8 * ((s + 1) * slots // 8 - s * slots // 8)
            for e in range(experts):
                w = d[WIN * e:WIN * (e + 1)]
                v = [w[:size]] if over[e] is None else [w[:8] + over[e], w[8:size]]
                over[e] = w[size:size + 8] if (s + 1) * slots % 8 else None
                if held[e] is not None:
                    v = [held[e], *v]
                v = jnp.concatenate(v, 0) if len(v) > 1 else v[0]
                k = v.shape[0] // 16 * 16
                z[e, pl.ds(done[e], k), :] = v[:k].astype(BF16)
                held[e] = v[k:] if k < v.shape[0] else None
                done[e] += k

    def chunk(n, last):
        _wait(xbuf, xsem)
        if not last:
            t2(n + 1)

            @pl.when(n + 2 < chunks)
            def _():
                t0(n + 2, 2)
        spread()
        for e in range(experts):
            side = (chunks + experts * n + e) % 2
            if e + 1 < experts:
                weights(n, e + 1, 1 - side)
            elif not last:
                weights(n + 1, 0, 1 - side)
            if last:
                have(side, 0)
                have(side, 1)
                half_rows = rows // 32 * 16 + 16

                def finish(j, _):
                    at = pl.ds(pl.multiple_of(512 * j, 512), 512)
                    at_u = pl.ds(pl.multiple_of(ff + 512 * j, 512), 512)
                    there = pl.ds(pl.multiple_of(j * rows, 16), rows)
                    if e > 0:
                        _wait(xbuf.at[there], hsem.at[j])
                    for lo, size in ((0, half_rows), (half_rows, rows - half_rows)):
                        r = pl.ds(lo, size)
                        g = acc[e, r, at] + _dot(z[e, r, :], wbuf[side, 0, :, at])
                        u = acc[e, r, at_u] + _dot(z[e, r, :], wbuf[side, 1, :, at])
                        v = (g * jax.nn.sigmoid(g) * u).astype(BF16)
                        xbuf[pl.ds(pl.multiple_of(j * rows + lo, 16), size), :] = v
                    pltpu.make_async_copy(xbuf.at[there], h.at[e, :, at], hsem.at[j]).start()
                    return 0

                lax.fori_loop(0, ff // 512, finish, 0)
            else:
                for half in range(2):
                    have(side, half)
                    at = pl.ds(half * ff, ff)
                    acc[e, :, at] += _dot(z[e], wbuf[side, half])
                    point = 2 * e + half
                    if point == 2:
                        @pl.when(n + 2 < chunks)
                        def _():
                            t1(n + 2)

                        @pl.when(n + 3 < chunks)
                        def _():
                            t0(n + 3, 0, 1)
                    if point == 3:
                        t3(n + 1)
                    if point == 4:
                        t4(n + 1)

    def most(n, _):
        chunk(n, False)
        return 0

    lax.fori_loop(0, chunks - 1, most, 0)
    chunk(chunks - 1, True)
    for k in range(ff // 512):
        _wait(xbuf.at[pl.ds(k * rows, rows)], hsem.at[k])
    meta_out.wait()
    _wait(mv.at[pl.ds(0, 15)], meta_send)
    _wait(xg.at[pl.ds(0, 15)], send_sem)


def _down_kernel(
    axis, chunks, experts, slots,
    h, hs, metag, wd, sd,
    y,
    hv, hsv, out32, wbuf, weight_t, mv, own, give, take, s1, s2, s3, r1, r2, r3, ost,
    hsem, lsem, wsem, give_sem, take_sem, credit, ss1, ss2, ss3, rs1, rs2, rs3, osem,
):
    me, bits, flip = _place(axis)
    tokens, rows = hs.shape[0], 16 * slots

    def cols(n):
        return pl.ds(pl.multiple_of(n * CB, CB), CB)

    def remote(src, dst, send, recv, mask):
        pltpu.make_async_remote_copy(
            src_ref=src, dst_ref=dst, send_sem=send, recv_sem=recv,
            device_id={axis: flip(mask)}, device_id_type=pl.DeviceIdType.MESH,
        ).start()

    def weights(n, e, side):
        src = wd.at[e, :, cols(n)] if e < experts else sd.at[:, cols(n)]
        pltpu.make_async_copy(src, wbuf.at[side], wsem.at[side]).start()

    copy = pltpu.make_async_copy(metag, mv, lsem)
    copy.start()
    pltpu.make_async_copy(h.at[0], hv.at[0], hsem.at[0]).start()
    weights(0, 0, 0)
    for e in range(1, experts):
        pltpu.make_async_copy(h.at[e], hv.at[e], hsem.at[e]).start()
    pltpu.make_async_copy(hs, hsv, hsem.at[experts]).start()
    _greet(axis, [flip(m) for m in (8, 4, 2, 1)])
    copy.wait()

    row = lax.broadcasted_iota(jnp.int32, (WIN, tokens), 0).astype(F32)
    rest = jnp.zeros((256 - experts * WIN, tokens), F32)

    def build(s, _):
        v = mv[s].astype(F32)
        shift = ((s * slots) % 8).astype(F32)
        hits = [
            jnp.where(v[e:e + 1, :] + shift == row, v[experts + e:experts + e + 1, :], 0.0) for e in range(experts)
        ]
        weight_t[s] = jnp.transpose(jnp.concatenate([*hits, rest], 0)).astype(BF16)
        return 0

    lax.fori_loop(0, 16, build, 0)
    for e in range(experts):
        out32[e, pl.ds(rows, 8), :] = jnp.zeros((8, CB), F32)

    def part(i):
        lo, size, dims = PARTS[i]
        return pl.ds(lo, size), dims

    def f32(ref, *at):
        return ref[at].astype(F32)

    def sum_at(n, block, r):
        p = n % LAG
        return own[p, block // 2, r, :] + f32(take, p, block // 2, r, slice(None))

    def free(n, ref, sem):
        @pl.when(n >= 2)
        def _():
            _wait(ref.at[n % 2], sem.at[n % 2])

    def stage1(n):
        p = n % 2
        _wait(take.at[n % LAG], take_sem.at[n % LAG])
        free(n, s1, ss1)
        for i in range(3):
            r, (a, b, c) = part(i)
            for k, q in enumerate((b + c, b, c, 0)):
                s1[p, k, r, :] = sum_at(n, q + a, r).astype(BF16)
                remote(s1.at[p, k, r], r1.at[n, k, r], ss1.at[p], rs1.at[n, i, k], a)

    def stage2(n):
        p = n % 2
        free(n, s2, ss2)
        for i in range(3):
            r, (a, b, c) = part(i)
            for k, q in enumerate((b + c, b)):
                _wait(r1.at[n, k, r], rs1.at[n, i, k])
                v = sum_at(n, q, r) + f32(r1, n, k, r, slice(None))
                s2[p, k, r, :] = v.astype(BF16)
                remote(s2.at[p, k, r], r2.at[n, k, r], ss2.at[p], rs2.at[n, i, k], b)

    def stage3(n):
        p = n % 2
        free(n, s3, ss3)
        for i in range(3):
            r, (a, b, c) = part(i)
            _wait(r1.at[n, 2, r], rs1.at[n, i, 2])
            _wait(r2.at[n, 0, r], rs2.at[n, i, 0])
            v = sum_at(n, c, r) + f32(r1, n, 2, r, slice(None)) + f32(r2, n, 0, r, slice(None))
            s3[p, r, :] = v.astype(BF16)
            remote(s3.at[p, r], r3.at[n, r], ss3.at[p], rs3.at[n, i], c)

    def stage4(n):
        p = n % 2
        free(n, ost, osem)
        for i in range(3):
            r, (a, b, c) = part(i)
            _wait(r1.at[n, 3, r], rs1.at[n, i, 3])
            _wait(r2.at[n, 1, r], rs2.at[n, i, 1])
            _wait(r3.at[n, r], rs3.at[n, i])
            v = sum_at(n, 0, r) + f32(r1, n, 3, r, slice(None)) + f32(r2, n, 1, r, slice(None))
            ost[p, r, :] = (v + f32(r3, n, r, slice(None))).astype(BF16)
        pltpu.make_async_copy(ost.at[p], y.at[:, cols(n)], osem.at[p]).start()
        pl.semaphore_signal(credit, inc=1, device_id={axis: flip(1)}, device_id_type=pl.DeviceIdType.MESH)

    def combine(r, core):
        s = flip(2 * r) - bits[1] + core
        at = pl.ds(pl.multiple_of(8 * ((s * slots) // 8), 8), WIN)
        rest = jnp.zeros((256 - experts * WIN, CB), F32)
        v = jnp.concatenate([*(out32[e, at, :] for e in range(experts)), rest], 0).astype(BF16)
        return _dot(weight_t[s], v)

    def late(n, k, stage):
        @pl.when((n >= k) & (n < chunks + k))
        def _():
            stage(n - k)

    def down(n, e):
        side = e % 2
        weights(n, e + 1, 1 - side)

        @pl.when(n == 0)
        def _():
            _wait(hv.at[e], hsem.at[e])

        _wait(wbuf.at[side], wsem.at[side])
        out32[e, pl.ds(0, rows), :] = _dot(hv[e], wbuf[side])

    def chunk(n, _):
        for e in range(experts):
            @pl.when(n < chunks)
            def _():
                down(n, e)

            if e == 0:
                late(n, 3, stage3)
                late(n, 1, stage1)
            if e == 1:
                late(n, 2, stage2)
            if e == 2:
                late(n, 3, stage4)

        @pl.when(n < chunks)
        def _():
            join(n)

        return 0

    def join(n):
        p = n % LAG

        @pl.when(n + 1 < chunks)
        def _():
            weights(n + 1, 0, 0)

        @pl.when(n >= 2)
        def _():
            _wait(give.at[n % 2], give_sem.at[n % 2])

        @pl.when(n >= LAG)
        def _():
            pl.semaphore_wait(credit, 1)

        for lo in (0, 4):
            for r in range(lo, lo + 4):
                give[n % 2, r] = combine(r, 1 - bits[1]).astype(BF16)
            some = pl.ds(lo, 4)
            remote(give.at[n % 2, some], take.at[p, some], give_sem.at[n % 2], take_sem.at[p], 1)

        @pl.when(n == 0)
        def _():
            _wait(hsv, hsem.at[experts])

        _wait(wbuf.at[1], wsem.at[1])
        own[p, 0] = combine(0, bits[1]) + _dot(hsv[...], wbuf[1])
        for r in range(1, 8):
            own[p, r] = combine(r, bits[1])

    lax.fori_loop(0, chunks + LAG, chunk, 0)
    for p in range(2):
        _wait(give.at[p], give_sem.at[p])
        _wait(s1.at[p], ss1.at[p])
        _wait(s2.at[p], ss2.at[p])
        _wait(s3.at[p], ss3.at[p])
        _wait(ost.at[p], osem.at[p])
    pl.semaphore_wait(credit, LAG)


def solution(mesh):
    axis, members = "ep", mesh.shape["ep"]

    def local(x, expert, slot, gate, w_gate, w_up, w_down, s_gate, s_up, s_down):
        x, expert, slot, gate = x[0, 0], expert[0, 0], slot[0, 0], gate[0, 0]
        tokens, d = x.shape
        expert, slot, gate = expert.T, slot.T, gate.T
        experts, _, ff = w_gate.shape
        slots = 5 * tokens * expert.shape[0] // (4 * experts * members)
        rows = members * slots
        hbm, dma, vmem = pl.BlockSpec(memory_space=pl.ANY), pltpu.SemaphoreType.DMA, pltpu.VMEM
        table, chunks = (members, 16, tokens), d // CW
        _, metag, h, hs = pl.pallas_call(
            functools.partial(_up_kernel, axis, chunks, experts, slots),
            name="gather_up",
            out_shape=(
                jax.ShapeDtypeStruct((members, tokens, d), BF16),
                jax.ShapeDtypeStruct(table, BF16),
                jax.ShapeDtypeStruct((experts, rows, ff), BF16),
                jax.ShapeDtypeStruct((tokens, ff), BF16),
            ),
            in_specs=[hbm] * 8,
            out_specs=(hbm,) * 4,
            scratch_shapes=[
                vmem((members * tokens, CW), BF16),
                vmem((experts, rows, CW), BF16),
                vmem((experts, rows, 2 * ff), F32),
                vmem((2, 2, CW, ff), BF16),
                vmem((members, experts * WIN, tokens), BF16),
                vmem(expert.shape, jnp.int32),
                vmem(slot.shape, jnp.int32),
                vmem(gate.shape, F32),
                vmem(table, BF16),
                vmem(table, BF16),
                dma, dma((chunks, 3, 3)), dma((chunks,)), dma, dma, dma((2, 2)), dma, dma, dma((3,)), dma((ff // 512,)),
            ],
            compiler_params=pltpu.CompilerParams(
                collective_id=0, has_side_effects=True, vmem_limit_bytes=VMEM_LIMIT
            ),
        )(x, expert, slot, gate, w_gate, w_up, s_gate, s_up)
        chunks = d // CB
        y = pl.pallas_call(
            functools.partial(_down_kernel, axis, chunks, experts, slots),
            name="down_scatter",
            out_shape=jax.ShapeDtypeStruct((tokens, d), BF16),
            in_specs=[hbm] * 5,
            out_specs=hbm,
            scratch_shapes=[
                vmem((experts, rows, ff), BF16),
                vmem((tokens, ff), BF16),
                vmem((experts, rows + 8, CB), F32),
                vmem((2, ff, CB), BF16),
                vmem((members, tokens, 256), BF16),
                vmem(table, BF16),
                vmem((LAG, 8, tokens, CB), F32),
                vmem((2, 8, tokens, CB), BF16),
                vmem((LAG, 8, tokens, CB), BF16),
                vmem((2, 4, tokens, CB), BF16),
                vmem((2, 2, tokens, CB), BF16),
                vmem((2, tokens, CB), BF16),
                vmem((chunks, 4, tokens, CB), BF16),
                vmem((chunks, 2, tokens, CB), BF16),
                vmem((chunks, tokens, CB), BF16),
                vmem((2, tokens, CB), BF16),
                dma((experts + 1,)), dma, dma((2,)), dma((2,)), dma((LAG,)), pltpu.SemaphoreType.REGULAR,
                dma((2,)), dma((2,)), dma((2,)),
                dma((chunks, 3, 4)), dma((chunks, 3, 2)), dma((chunks, 3)), dma((2,)),
            ],
            compiler_params=pltpu.CompilerParams(
                collective_id=1, has_side_effects=True, vmem_limit_bytes=VMEM_LIMIT
            ),
        )(h, hs, metag, w_down, s_down)
        return y[None, None]

    tok = P("dp", "ep", None, None)
    own = P("ep", None, None)
    return jax.shard_map(
        local,
        mesh=mesh,
        in_specs=(tok, tok, tok, tok, own, own, own, P(), P(), P()),
        out_specs=tok,
        check_vma=False,
    )
```
